32 devices in a mesh: groups: 2 (over y), seq: 8 (over z, x), section: 2 (over core).
Axes of the slice: x: 2, y: 2, z: 4, core: 2. Of those that a mesh axis runs over, the one named last changes fastest.
Arguments:
- hidden_in: bfloat16 [4, 8192], P('groups', 'seq'), parts along dimension 0, may hold values from -40 to 40
- norm_gain: bfloat16 [2, 8192], P('section', 'seq'), may hold values from 0.5 to 1.5
- qkv_weight: bfloat16 [2, 8192, 10240], P('section', 'seq'), as said below
- out_weight: bfloat16 [2, 8192, 8192], P('section', None, 'seq'), may hold values from -0.0625 to 0.0625
- memory: bfloat16 [2, 4, 8, 32, 2, 128, 128], P('section', 'groups', None, 'seq'), parts along dimension 1, may hold values from -12 to 12
- lengths: int32 [4], P('groups'), parts along dimension 0, may hold values from 2048 to 4096
- selected: int32 [4, 8, 16], P('groups'), parts along dimension 0, may hold values from 0 to 31, all different within a row
Outputs:
- hidden_out: bfloat16 [2, 4, 8192], P('section', 'groups', 'seq'), parts along dimension 1
- attention: bfloat16 [2, 4, 8192], P('section', 'groups'), parts along dimension 1
The draws below stay inside these ranges and needn't reach their ends.
There are 2 independent parts, one for each index of `groups`. The reference program is written for one: setup_inputs(seed, part) draws one part's arguments, and reference() takes and returns one part's arrays. A program takes and returns all parts, laid end to end along the dimension named above; an argument that names none is the same for every part. Nothing has to cross between parts.
Inputs may be any that keep to these rules, and one draw needn't show every extreme that they name: `selected`: for each sequence and key-value head the 16 block numbers differ. `qkv_weight`: every entry's magnitude is at most 256 / sqrt(8192).
All inputs are finite; a program needn't handle non-finite values.
Results may differ from the reference program's by a relative error of at most 0.025.
The reference program's roundings to bfloat16 on the way count: a program that leaves them out, or rounds other values in their place, can miss the bound.
Values may be sent and summed in bfloat16 or wider, within the bound.
A program may use at most 128 MiB of HBM per device.

```python
import jax
import jax.numpy as jnp
from jax import lax

D = 8192
HEADS = 64
KVH = 8
HEAD = 128
BLOCK = 128
SEL = 16
SEQS = 2
NBLK = 32
LAYERS = 2
QKVW = 10240


def draw_qkv_weight(key, part):
    base_draw = jax.random.normal(key, (LAYERS, D, QKVW), jnp.float32)
    base_draw = jnp.clip(base_draw, -4.0, 4.0) * D ** (-0.5)
    return base_draw.astype(jnp.bfloat16)


def draw_hidden_in(key, part):
    column_pos = jnp.arange(D, dtype=jnp.float32) / max(D - 1, 1)
    base_draw = jnp.clip(jax.random.normal(key, (SEQS, D), jnp.float32), -5.0, 5.0)
    column_scale = jnp.exp(jnp.log(4.0) * column_pos)
    base_draw = base_draw * column_scale[None, :] * 0.5
    return jnp.clip(base_draw, -40.0, 40.0).astype(jnp.bfloat16)


def level_of(stream_key, dims, shards, low, top_value):
    def one(axis_at, parts):
        heights = jax.random.uniform(jax.random.fold_in(jax.random.fold_in(stream_key, 6), axis_at), (parts,), jnp.float32, low / len(shards), top_value / len(shards))
        return jnp.repeat(jnp.exp(heights), dims[axis_at] // parts).reshape((-1,) + (1,) * (len(dims) - axis_at - 1))

    factor_of = one(*shards[0])
    for cut in shards[1:]:
        factor_of = factor_of * one(*cut)
    return factor_of


def different_ones(own_key, rows, number_of, top, lift):
    order = jax.random.permutation(jax.random.fold_in(own_key, 1), number_of)
    favour = order
    for power in range(3):
        favour = favour * favour // number_of
    favour = favour * lift // number_of
    chance = jax.random.randint(jax.random.fold_in(own_key, 2), (rows, number_of), 0, 4096) + favour
    holders = jax.random.permutation(jax.random.fold_in(own_key, 3), rows)[jnp.arange(number_of) % rows]
    chance = jnp.where(jnp.arange(rows)[:, None] == holders[None, :], 1 << 14, chance)
    merit = chance * number_of + jnp.arange(number_of)
    return lax.top_k(merit.astype(jnp.int32), top)[1].astype(jnp.int32)


def gaussian(rng, dims, width, reach, pieces=(), held_as=jnp.bfloat16):
    entries = width * jax.random.normal(rng, dims, jnp.float32)
    if pieces:
        entries = entries * level_of(rng, dims, pieces, -0.22, 0.18)
    return jnp.clip(entries, -reach, reach).astype(held_as)


def setup_inputs(seed: int = 0, part: int = 0) -> dict:
    splits = jax.random.split(jax.random.key(seed), 8)
    part_splits = jax.random.split(jax.random.fold_in(splits[7], part), 8)
    hidden_in = draw_hidden_in(jax.random.fold_in(jax.random.fold_in(splits[7], part), 71), part)
    norm_gain = jnp.clip(1.0 + 0.1 * jax.random.normal(splits[1], (LAYERS, D), jnp.float32), 0.5, 1.5).astype(jnp.bfloat16)
    qkv_weight = draw_qkv_weight(jax.random.fold_in(splits[7], 71), part)
    out_weight = gaussian(splits[3], (LAYERS, HEADS * HEAD, D), (HEADS * HEAD) ** -0.5, 0.0625, ((0, 2), (2, 8)))
    memory = gaussian(part_splits[4], (LAYERS, SEQS, KVH, NBLK, 2, BLOCK, HEAD), 2.0, 12.0, ((0, 2), (3, 8)))
    lengths = jax.random.randint(part_splits[5], (SEQS,), NBLK * BLOCK // 2, NBLK * BLOCK + 1).astype(jnp.int32)
    selected = different_ones(part_splits[6], SEQS * KVH, NBLK, SEL, 8192).reshape((SEQS, KVH, SEL))
    return {"hidden_in": hidden_in, "norm_gain": norm_gain, "qkv_weight": qkv_weight, "out_weight": out_weight, "memory": memory, "lengths": lengths, "selected": selected}


EPSILON = 1e-05
FLOOR = -1e+30

def pick_blocks(layer_memory, chosen_ids):
    return jax.vmap(jax.vmap(lambda blocks, ids: blocks[ids]))(layer_memory, chosen_ids)

def reference(hidden_in, norm_gain, qkv_weight, out_weight, memory, lengths, selected):
    heads_total = HEADS * HEAD
    kv_width = KVH * HEAD
    group_size = HEADS // KVH
    score_scale = HEAD ** (-0.5)
    offsets = jnp.arange(BLOCK, dtype=jnp.int32)
    positions = (selected[..., None] * BLOCK + offsets).reshape(SEQS, KVH, SEL * BLOCK)
    live_mask = positions < lengths[:, None, None]
    current = hidden_in
    hidden_list = []
    attention_list = []
    for layer_index in range(LAYERS):
        hidden_wide = current.astype(jnp.float32)
        squares = lax.optimization_barrier(jnp.sum(hidden_wide * hidden_wide, axis=1))
        normed = (hidden_wide * norm_gain[layer_index].astype(jnp.float32)).astype(jnp.bfloat16)
        summed = jnp.dot(normed, qkv_weight[layer_index], preferred_element_type=jnp.float32)
        projected = (summed * lax.rsqrt(squares / D + EPSILON)[:, None]).astype(jnp.bfloat16)
        queries = projected[:, :heads_total].reshape(SEQS, KVH, group_size, HEAD).astype(jnp.float32)
        new_keys = projected[:, heads_total:heads_total + kv_width].reshape(SEQS, KVH, HEAD).astype(jnp.float32)
        new_values = projected[:, heads_total + kv_width:].reshape(SEQS, KVH, HEAD).astype(jnp.float32)
        picked = pick_blocks(memory[layer_index], selected)
        cache_keys = picked[:, :, :, 0].reshape(SEQS, KVH, SEL * BLOCK, HEAD).astype(jnp.float32)
        cache_values = picked[:, :, :, 1].reshape(SEQS, KVH, SEL * BLOCK, HEAD).astype(jnp.float32)
        scores = jnp.einsum('bgrd,bgnd->bgrn', queries, cache_keys, precision=lax.Precision.HIGHEST) * score_scale
        own_score = jnp.einsum('bgrd,bgd->bgr', queries, new_keys, precision=lax.Precision.HIGHEST) * score_scale
        masked = jnp.where(live_mask[:, :, None, :], scores, FLOOR)
        top_score = jnp.maximum(lax.optimization_barrier(jnp.max(masked, axis=3)), own_score)
        weights = jnp.where(live_mask[:, :, None, :], jnp.exp(masked - top_score[..., None]), 0.0)
        own_weight = jnp.exp(own_score - top_score)
        denominator = lax.optimization_barrier(jnp.sum(weights, axis=3)) + own_weight
        numerator = jnp.einsum('bgrn,bgnd->bgrd', weights, cache_values, precision=lax.Precision.HIGHEST)
        numerator = numerator + own_weight[..., None] * new_values[:, :, None, :]
        attended = (numerator / denominator[..., None]).astype(jnp.bfloat16).reshape(SEQS, heads_total)
        branch = jnp.dot(attended, out_weight[layer_index], preferred_element_type=jnp.float32)
        current = (hidden_wide + branch).astype(jnp.bfloat16)
        hidden_list.append(current)
        attention_list.append(attended)
    return (jnp.stack(hidden_list), jnp.stack(attention_list))
```

```python
import functools

import jax
import jax.numpy as jnp
from jax import lax
from jax.experimental import pallas as pl
from jax.experimental.pallas import tpu as pltpu
from jax.sharding import PartitionSpec as P

D = 8192
HEADS = 64
KVH = 8
HEAD = 128
BLOCK = 128
GROUP = HEADS // KVH
GW = GROUP * HEAD
EPSILON = 1e-05
FLOOR = -1e30
MESH = pl.DeviceIdType.MESH


def kernel(
    seq_count,
    section_count,
    hidden_ref,
    gain_ref,
    lengths_ref,
    selected_ref,
    qkv_hbm,
    out_hbm,
    memory_hbm,
    hidden_out,
    attention_out,
    w_q,
    w_kv,
    w_o,
    cache,
    hidden,
    hidden_send,
    live,
    part,
    part_kv,
    got,
    got_kv,
    own_q,
    q_all,
    stats,
    got_stats,
    att_all,
    att_wide,
    w_sem,
    kv_sem,
    o_sem,
    cache_sem,
    hid_sems,
    part_send,
    part_recv,
    partkv_send,
    partkv_recv,
    q_send,
    q_recv,
    st_send,
    st_recv,
    att_send,
    att_recv,
):
    me = lax.axis_index("seq")
    section = lax.axis_index("section")
    ratio = seq_count // KVH
    home = me // ratio
    seqs = hidden_ref.shape[0]
    width = hidden_ref.shape[1]
    blocks_local = memory_hbm.shape[3]
    tokens = blocks_local * BLOCK
    score_scale = HEAD ** (-0.5)
    order = [lax.rem(home + 1 + i, KVH) for i in range(KVH)]

    def when_owner(fn):
        if ratio == 1:
            fn()
        else:
            pl.when(me == home * ratio)(fn)

    def when_not_owner(fn):
        if ratio != 1:
            pl.when(me != home * ratio)(fn)

    def peer(i):
        return lax.rem(me + i, seq_count)

    def remote(src, dst, send, recv, target):
        return pltpu.make_async_remote_copy(
            src_ref=src,
            dst_ref=dst,
            send_sem=send,
            recv_sem=recv,
            device_id={"seq": target},
            device_id_type=MESH,
        )

    w_copies = []
    for i, g in enumerate(order):
        c = pltpu.make_async_copy(
            qkv_hbm.at[0, :, pl.ds(pl.multiple_of(g * GW, GW), GW)], w_q.at[i], w_sem.at[i]
        )
        c.start()
        w_copies.append(c)
    kv_copy = pltpu.make_async_copy(
        qkv_hbm.at[0, :, pl.ds(HEADS * HEAD, 2 * KVH * HEAD)], w_kv, kv_sem
    )
    kv_copy.start()
    cache_copy = pltpu.make_async_copy(memory_hbm.at[0], cache, cache_sem)
    cache_copy.start()
    o_copies = []
    for g in range(KVH):
        o_copies.append(
            pltpu.make_async_copy(out_hbm.at[0, pl.ds(g * GW, GW), :], w_o.at[g], o_sem.at[g])
        )
        o_copies[g].start()

    barrier = pltpu.get_barrier_semaphore()
    for i in range(1, seq_count):
        pl.semaphore_signal(barrier, inc=1, device_id={"seq": peer(i)}, device_id_type=MESH)
    for i in range(1, section_count):
        pl.semaphore_signal(
            barrier,
            inc=1,
            device_id={"section": lax.rem(section + i, section_count)},
            device_id_type=MESH,
        )

    offsets = lax.broadcasted_iota(jnp.int32, (KVH, BLOCK), 1)
    for b in range(seqs):
        ids = selected_ref[b]
        for t in range(blocks_local):
            block = me * blocks_local + t
            hit = jnp.max(jnp.where(ids == block, 1.0, 0.0), axis=1, keepdims=True)
            inside = jnp.where(block * BLOCK + offsets < lengths_ref[b], 1.0, 0.0)
            live[b, :, t * BLOCK : (t + 1) * BLOCK] = hit * inside

    pl.semaphore_wait(barrier, seq_count - 1 + section_count - 1)

    def next_section_copy(target):
        return pltpu.make_async_remote_copy(
            src_ref=hidden_send,
            dst_ref=hidden,
            send_sem=hid_sems.at[0],
            recv_sem=hid_sems.at[1],
            device_id={"section": target},
            device_id_type=MESH,
        )

    @pl.when(section == 0)
    def _():
        hidden[...] = hidden_ref[...].astype(jnp.float32)

    @pl.when(section > 0)
    def _():
        next_section_copy(lax.rem(section + 1, section_count)).wait_recv()

    wide = hidden[...]
    normed = (wide * gain_ref[...].astype(jnp.float32)).astype(jnp.bfloat16)
    squared = wide * wide
    squares = squared[:, :HEAD]
    for t in range(1, width // HEAD):
        squares = squares + squared[:, t * HEAD : (t + 1) * HEAD]

    sends = []
    for i, g in enumerate(order):
        w_copies[i].wait()
        acc = jnp.dot(normed, w_q[i], preferred_element_type=jnp.float32)
        owner = g * ratio

        def store(ref):
            ref[:, :GW] = acc
            ref[:, GW:] = squares

        if i < KVH - 1:
            store(part.at[i])
            c = remote(part.at[i], got.at[me], part_send.at[i], part_recv.at[me], owner)
            c.start()
            sends.append(c)
        else:
            when_owner(functools.partial(store, got.at[me]))

            def send_home():
                store(part.at[i])
                remote(part.at[i], got.at[me], part_send.at[i], part_recv.at[me], owner).start()

            when_not_owner(send_home)

    kv_copy.wait()
    acc_kv = jnp.dot(normed, w_kv[...], preferred_element_type=jnp.float32)
    for g in range(KVH):
        part_kv[g, :, :HEAD] = acc_kv[:, g * HEAD : (g + 1) * HEAD]
        part_kv[g, :, HEAD:] = acc_kv[:, (KVH + g) * HEAD : (KVH + g + 1) * HEAD]
    for i in range(KVH - 1):
        g = order[i]
        c = remote(
            part_kv.at[g], got_kv.at[me], partkv_send.at[i], partkv_recv.at[me], g * ratio
        )
        c.start()
        sends.append(c)

    def kv_home():
        got_kv[me] = part_kv[home]

    def kv_away():
        remote(
            part_kv.at[home],
            got_kv.at[me],
            partkv_send.at[KVH - 1],
            partkv_recv.at[me],
            home * ratio,
        ).start()

    when_owner(kv_home)
    when_not_owner(kv_away)

    def project_own():
        for i in range(1, seq_count):
            s = peer(i)
            remote(part.at[0], got.at[s], part_send.at[0], part_recv.at[s], s).wait_recv()
        total = got[0]
        for s in range(1, seq_count):
            total = total + got[s]
        square_sum = jnp.sum(total[:, GW:], axis=1, keepdims=True)
        scale = lax.rsqrt(square_sum / D + EPSILON)
        projected = (total[:, :GW] * scale).astype(jnp.bfloat16).astype(jnp.float32)
        for h in range(GROUP):
            own_q[pl.ds(h, seqs, stride=GROUP), :] = projected[:, h * HEAD : (h + 1) * HEAD]
        own_q[seqs * GROUP : seqs * GROUP + seqs, :] = jnp.broadcast_to(scale, (seqs, HEAD))
        q_all[home] = own_q[: seqs * GROUP, :].astype(jnp.bfloat16)
        for i in range(1, seq_count):
            remote(
                q_all.at[home], q_all.at[home], q_send.at[i], q_recv.at[home], peer(i)
            ).start()

    when_owner(project_own)

    cache_copy.wait()
    lanes = lax.broadcasted_iota(jnp.int32, (GROUP, HEAD), 1)

    def wait_q(g):
        remote(q_all.at[g], q_all.at[g], q_send.at[0], q_recv.at[g], peer(1)).wait_recv()

    for i, g in enumerate(order):
        if i < KVH - 1:
            wait_q(g)
        else:
            when_not_owner(functools.partial(wait_q, g))
        queries = q_all[g]
        outs, peaks, totals = [], [], []
        for b in range(seqs):
            keys = cache[b, g, :, 0].reshape(tokens, HEAD)
            values = cache[b, g, :, 1].reshape(tokens, HEAD)
            scores = lax.dot_general(
                queries, keys, (((1,), (1,)), ((), ())), preferred_element_type=jnp.float32
            )
            scores = scores[b * GROUP : (b + 1) * GROUP] * score_scale
            alive = live[b, pl.ds(g, 1), :] > 0.5
            masked = jnp.where(alive, scores, FLOOR)
            peak = jnp.max(masked, axis=1, keepdims=True)
            weight = jnp.where(alive, jnp.exp(masked - peak), 0.0)
            high = weight.astype(jnp.bfloat16).astype(jnp.float32)
            both = jnp.concatenate([high, weight - high], axis=0).astype(jnp.bfloat16)
            out = jnp.dot(both, values, preferred_element_type=jnp.float32)
            outs.append(out[:GROUP] + out[GROUP:])
            peaks.append(peak)
            totals.append(jnp.sum(weight, axis=1, keepdims=True))
        packed = jnp.zeros((GROUP, HEAD), jnp.float32)
        for b in range(seqs):
            packed = jnp.where(lanes == 2 * b, peaks[b], packed)
            packed = jnp.where(lanes == 2 * b + 1, totals[b], packed)

        def put(ref):
            for b in range(seqs):
                ref[b] = outs[b]
            ref[seqs] = packed

        def send_stats():
            put(stats.at[i])
            c = remote(stats.at[i], got_stats.at[me], st_send.at[i], st_recv.at[me], g * ratio)
            c.start()
            return c

        if i < KVH - 1:
            sends.append(send_stats())
        else:
            when_owner(functools.partial(put, got_stats.at[me]))
            when_not_owner(lambda: send_stats() and None)

    def finish_own():
        for i in range(1, seq_count):
            s = peer(i)
            remote(
                part_kv.at[0], got_kv.at[s], partkv_send.at[0], partkv_recv.at[s], s
            ).wait_recv()
        new_kv = got_kv[0]
        for s in range(1, seq_count):
            new_kv = new_kv + got_kv[s]
        scale = own_q[seqs * GROUP : seqs * GROUP + seqs, :][:, :1]
        new_kv = (new_kv * scale).astype(jnp.bfloat16).astype(jnp.float32)
        own_scores = []
        for b in range(seqs):
            query = own_q[b * GROUP : (b + 1) * GROUP, :]
            own_scores.append(
                jnp.sum(query * new_kv[b : b + 1, :HEAD], axis=1, keepdims=True) * score_scale
            )
        for i in range(1, seq_count):
            s = peer(i)
            remote(stats.at[0], got_stats.at[s], st_send.at[0], st_recv.at[s], s).wait_recv()
        rows = []
        packed = [got_stats[s, seqs] for s in range(seq_count)]
        for b in range(seqs):
            top = own_scores[b]
            for s in range(seq_count):
                top = jnp.maximum(top, packed[s][:, 2 * b : 2 * b + 1])
            own_weight = jnp.exp(own_scores[b] - top)
            denominator = own_weight
            numerator = own_weight * new_kv[b : b + 1, HEAD:]
            for s in range(seq_count):
                factor = jnp.exp(packed[s][:, 2 * b : 2 * b + 1] - top)
                denominator = denominator + packed[s][:, 2 * b + 1 : 2 * b + 2] * factor
                numerator = numerator + got_stats[s, b] * factor
            rows.append(numerator / denominator)
        att_all[home] = jnp.concatenate(rows, axis=0).astype(jnp.bfloat16)
        for i in range(1, seq_count):
            remote(
                att_all.at[home], att_all.at[home], att_send.at[i], att_recv.at[home], peer(i)
            ).start()

    when_owner(finish_own)

    def wait_att(g):
        remote(att_all.at[g], att_all.at[g], att_send.at[0], att_recv.at[g], peer(1)).wait_recv()

    for g in range(KVH):
        o_copies[g].wait()
    branch = jnp.zeros((seqs, width), jnp.float32)
    for i in range(KVH):
        g = lax.rem(home + i, KVH)
        if i > 0:
            wait_att(g)
        else:
            when_not_owner(functools.partial(wait_att, g))
        att_wide[i] = att_all[g].astype(jnp.float32)
        attended = jnp.concatenate(
            [att_wide[i, pl.ds(h, seqs, stride=GROUP), :] for h in range(GROUP)], axis=1
        ).astype(jnp.bfloat16)
        attention_out[0, :, pl.ds(pl.multiple_of(g * GW, GW), GW)] = attended
        branch = branch + jnp.dot(attended, w_o[g], preferred_element_type=jnp.float32)
    new_hidden = (hidden[...] + branch).astype(jnp.bfloat16)
    hidden_out[0] = new_hidden

    @pl.when(section < section_count - 1)
    def _():
        hidden_send[...] = new_hidden.astype(jnp.float32)
        c = next_section_copy(section + 1)
        c.start()
        c.wait_send()

    for c in sends:
        c.wait_send()

    def drain_owner():
        for i in range(1, seq_count):
            remote(
                q_all.at[home], q_all.at[home], q_send.at[i], q_recv.at[home], peer(i)
            ).wait_send()
            remote(
                att_all.at[home], att_all.at[home], att_send.at[i], att_recv.at[home], peer(i)
            ).wait_send()

    def drain_other():
        last = KVH - 1
        to = home * ratio
        remote(part.at[last], got.at[me], part_send.at[last], part_recv.at[me], to).wait_send()
        remote(
            part_kv.at[home], got_kv.at[me], partkv_send.at[last], partkv_recv.at[me], to
        ).wait_send()
        remote(
            stats.at[last], got_stats.at[me], st_send.at[last], st_recv.at[me], to
        ).wait_send()

    when_owner(drain_owner)
    when_not_owner(drain_other)


def body(hidden_in, norm_gain, qkv_weight, out_weight, memory, lengths, selected):
    seq_count = lax.axis_size("seq")
    section_count = lax.axis_size("section")
    seqs, width = hidden_in.shape
    blocks_local = memory.shape[3]
    dma = pltpu.SemaphoreType.DMA
    vmem = pl.BlockSpec(memory_space=pltpu.VMEM)
    anywhere = pl.BlockSpec(memory_space=pl.ANY)
    return pl.pallas_call(
        functools.partial(kernel, seq_count, section_count),
        out_shape=(
            jax.ShapeDtypeStruct((1, seqs, width), jnp.bfloat16),
            jax.ShapeDtypeStruct((1, seqs, HEADS * HEAD), jnp.bfloat16),
        ),
        in_specs=[
            vmem,
            vmem,
            pl.BlockSpec(memory_space=pltpu.SMEM),
            vmem,
            anywhere,
            anywhere,
            anywhere,
        ],
        out_specs=(vmem, vmem),
        scratch_shapes=[
            pltpu.VMEM((KVH, width, GW), jnp.bfloat16),
            pltpu.VMEM((width, 2 * KVH * HEAD), jnp.bfloat16),
            pltpu.VMEM((KVH, GW, width), jnp.bfloat16),
            pltpu.VMEM((seqs, KVH, blocks_local, 2, BLOCK, HEAD), jnp.bfloat16),
            pltpu.VMEM((seqs, width), jnp.float32),
            pltpu.VMEM((seqs, width), jnp.float32),
            pltpu.VMEM((seqs, KVH, blocks_local * BLOCK), jnp.float32),
            pltpu.VMEM((KVH, seqs, GW + HEAD), jnp.float32),
            pltpu.VMEM((KVH, seqs, 2 * HEAD), jnp.float32),
            pltpu.VMEM((seq_count, seqs, GW + HEAD), jnp.float32),
            pltpu.VMEM((seq_count, seqs, 2 * HEAD), jnp.float32),
            pltpu.VMEM((seqs * GROUP + 8, HEAD), jnp.float32),
            pltpu.VMEM((KVH, seqs * GROUP, HEAD), jnp.bfloat16),
            pltpu.VMEM((KVH, seqs + 1, GROUP, HEAD), jnp.float32),
            pltpu.VMEM((seq_count, seqs + 1, GROUP, HEAD), jnp.float32),
            pltpu.VMEM((KVH, seqs * GROUP, HEAD), jnp.bfloat16),
            pltpu.VMEM((KVH, seqs * GROUP, HEAD), jnp.float32),
            dma((KVH,)),
            dma,
            dma((KVH,)),
            dma,
            dma((2,)),
            dma((KVH,)),
            dma((seq_count,)),
            dma((KVH,)),
            dma((seq_count,)),
            dma((seq_count,)),
            dma((KVH,)),
            dma((KVH,)),
            dma((seq_count,)),
            dma((seq_count,)),
            dma((KVH,)),
        ],
        compiler_params=pltpu.CompilerParams(
            collective_id=0, has_side_effects=True, vmem_limit_bytes=56 * 1024 * 1024
        ),
    )(hidden_in, norm_gain, lengths, selected, qkv_weight, out_weight, memory)


def solution(mesh):
    return jax.shard_map(
        body,
        mesh=mesh,
        in_specs=(
            P("groups", "seq"),
            P("section", "seq"),
            P("section", "seq", None),
            P("section", None, "seq"),
            P("section", "groups", None, "seq", None, None, None),
            P("groups"),
            P("groups", None, None),
        ),
        out_specs=(P("section", "groups", "seq"), P("section", "groups", None)),
        check_vma=False,
    )
```

```python
import functools

import jax
import jax.numpy as jnp
from jax import lax
from jax.experimental import pallas as pl
from jax.experimental.pallas import tpu as pltpu
from jax.sharding import PartitionSpec as P

D = 8192
HEADS = 64
KVH = 8
HEAD = 128
BLOCK = 128
GROUP = HEADS // KVH
GW = GROUP * HEAD
EPSILON = 1e-05
FLOOR = -1e30
MESH = pl.DeviceIdType.MESH
OWNERS = 4
EACH = KVH // OWNERS
ROUNDS = ((3,), (2, 1), (0,))
OUTPUT_ROUNDS = ((3,), (2,), (1,), (0,))


def kernel(
    seq_count,
    section_count,
    hidden_ref,
    gain_ref,
    lengths_ref,
    selected_ref,
    qkv_hbm,
    out_hbm,
    memory_hbm,
    hidden_out,
    attention_out,
    w_q,
    w_kv,
    w_o,
    cache,
    hidden,
    hidden_send,
    live,
    part,
    part_kv,
    got,
    got_kv,
    own_q,
    q_all,
    stats,
    got_stats,
    att_all,
    att_wide,
    w_sem,
    kv_sem,
    o_sem,
    cache_sem,
    hid_sems,
    part_send,
    part_recv,
    partkv_send,
    partkv_recv,
    q_send,
    q_recv,
    st_send,
    st_recv,
    att_send,
    att_recv,
):
    me = lax.axis_index("seq")
    section = lax.axis_index("section")
    first = seq_count // 2 - OWNERS // 2
    home = lax.rem(me + seq_count - first, seq_count)
    half = me // (seq_count // 2)
    side = lax.rem(me, 2)
    seqs = hidden_ref.shape[0]
    width = hidden_ref.shape[1]
    blocks_local = memory_hbm.shape[3]
    tokens = blocks_local * BLOCK
    score_scale = HEAD ** (-0.5)
    order = [
        2 * (1 - half) + 1 - side,
        2 * (1 - half) + side,
        2 * half + 1 - side,
        2 * half + side,
    ]
    is_owner = home < OWNERS

    def when_owner(fn):
        pl.when(is_owner)(fn)

    def when_not_owner(fn):
        pl.when(home >= OWNERS)(fn)

    def peer(i):
        return lax.rem(me + i, seq_count)

    def remote(src, dst, send, recv, target):
        return pltpu.make_async_remote_copy(
            src_ref=src,
            dst_ref=dst,
            send_sem=send,
            recv_sem=recv,
            device_id={"seq": target},
            device_id_type=MESH,
        )

    w_copies = []
    for i in range(KVH):
        g = order[i // EACH] * EACH + i % EACH
        c = pltpu.make_async_copy(
            qkv_hbm.at[0, :, pl.ds(pl.multiple_of(g * GW, GW), GW)], w_q.at[i], w_sem.at[i]
        )
        c.start()
        w_copies.append(c)
    kv_copy = pltpu.make_async_copy(
        qkv_hbm.at[0, :, pl.ds(HEADS * HEAD, 2 * KVH * HEAD)], w_kv, kv_sem
    )
    kv_copy.start()
    cache_copy = pltpu.make_async_copy(memory_hbm.at[0], cache, cache_sem)
    o_copies = []
    for o in range(OWNERS):
        rows_of = pl.ds(o * EACH * GW, EACH * GW)
        o_copies.append(
            pltpu.make_async_copy(out_hbm.at[0, rows_of, :], w_o.at[o], o_sem.at[o])
        )

    barrier = pltpu.get_barrier_semaphore()
    for i in range(1, seq_count):
        pl.semaphore_signal(barrier, inc=1, device_id={"seq": peer(i)}, device_id_type=MESH)
    for i in range(1, section_count):
        pl.semaphore_signal(
            barrier,
            inc=1,
            device_id={"section": lax.rem(section + i, section_count)},
            device_id_type=MESH,
        )

    offsets = lax.broadcasted_iota(jnp.int32, (KVH, BLOCK), 1)
    for b in range(seqs):
        ids = selected_ref[b]
        for t in range(blocks_local):
            block = me * blocks_local + t
            hit = jnp.max(jnp.where(ids == block, 1.0, 0.0), axis=1, keepdims=True)
            inside = jnp.where(block * BLOCK + offsets < lengths_ref[b], 1.0, 0.0)
            live[b, :, t * BLOCK : (t + 1) * BLOCK] = hit * inside

    pl.semaphore_wait(barrier, seq_count - 1 + section_count - 1)

    def next_section_copy(target):
        return pltpu.make_async_remote_copy(
            src_ref=hidden_send,
            dst_ref=hidden,
            send_sem=hid_sems.at[0],
            recv_sem=hid_sems.at[1],
            device_id={"section": target},
            device_id_type=MESH,
        )

    @pl.when(section == 0)
    def _():
        hidden[...] = hidden_ref[...].astype(jnp.float32)

    @pl.when(section > 0)
    def _():
        next_section_copy(lax.rem(section + 1, section_count)).wait_recv()

    wide = hidden[...]
    normed = (wide * gain_ref[...].astype(jnp.float32)).astype(jnp.bfloat16)
    squared = wide * wide
    squares = squared[:, :HEAD]
    for t in range(1, width // HEAD):
        squares = squares + squared[:, t * HEAD : (t + 1) * HEAD]

    sends = []
    last = OWNERS - 1

    def part_copy(i):
        return remote(
            part.at[i], got.at[me], part_send.at[i], part_recv.at[me], first + order[i]
        )

    for i in range(OWNERS):
        pieces = []
        for j in range(i * EACH, (i + 1) * EACH):
            w_copies[j].wait()
            if j == KVH // 2:
                cache_copy.start()
            if j == KVH - 1:
                for c in o_copies:
                    c.start()
            pieces.append(jnp.dot(normed, w_q[j], preferred_element_type=jnp.float32))

        def store(ref):
            for j in range(EACH):
                ref[:, j * GW : (j + 1) * GW] = pieces[j]
            ref[:, EACH * GW :] = squares

        if i < last:
            store(part.at[i])
            c = part_copy(i)
            c.start()
            sends.append(c)
        else:

            def send_last():
                store(part.at[i])
                part_copy(i).start()

            when_owner(functools.partial(store, got.at[me]))
            when_not_owner(send_last)

    kv_copy.wait()
    acc_kv = jnp.dot(normed, w_kv[...], preferred_element_type=jnp.float32)
    span = EACH * HEAD
    for o in range(OWNERS):
        part_kv[o, :, :span] = acc_kv[:, o * span : (o + 1) * span]
        part_kv[o, :, span:] = acc_kv[:, KVH * HEAD + o * span : KVH * HEAD + (o + 1) * span]

    def kv_part_copy(i):
        return remote(
            part_kv.at[order[i]],
            got_kv.at[me],
            partkv_send.at[i],
            partkv_recv.at[me],
            first + order[i],
        )

    for i in range(last):
        c = kv_part_copy(i)
        c.start()
        sends.append(c)

    def kv_home():
        got_kv[me] = part_kv[order[last]]

    when_owner(kv_home)
    when_not_owner(lambda: kv_part_copy(last).start())

    def project_own():
        for i in range(1, seq_count):
            s = peer(i)
            remote(part.at[0], got.at[s], part_send.at[0], part_recv.at[s], s).wait_recv()
        total = got[0]
        for s in range(1, seq_count):
            total = total + got[s]
        square_sum = jnp.sum(total[:, EACH * GW :], axis=1, keepdims=True)
        scale = lax.rsqrt(square_sum / D + EPSILON)
        projected = (total[:, : EACH * GW] * scale).astype(jnp.bfloat16).astype(jnp.float32)
        for j in range(EACH):
            for h in range(GROUP):
                at = (j * GROUP + h) * HEAD
                own_q[pl.ds(j * seqs * GROUP + h, seqs, stride=GROUP), :] = projected[
                    :, at : at + HEAD
                ]
        q_rows = EACH * seqs * GROUP
        own_q[q_rows : q_rows + seqs, :] = jnp.broadcast_to(scale, (seqs, HEAD))
        q_all[order[last]] = own_q[:q_rows, :].astype(jnp.bfloat16)
        for i in range(1, seq_count):
            remote(
                q_all.at[order[last]], q_all.at[order[last]], q_send.at[i], q_recv.at[order[last]], peer(i)
            ).start()

    when_owner(project_own)

    cache_copy.wait()
    lanes = lax.broadcasted_iota(jnp.int32, (GROUP, HEAD), 1)

    def wait_q(g):
        remote(q_all.at[g], q_all.at[g], q_send.at[0], q_recv.at[g], peer(1)).wait_recv()

    def attend(owners):
        pairs = [(o, j, b) for o in owners for j in range(EACH) for b in range(seqs)]
        all_scores = []
        for o, j, b in pairs:
            queries = q_all[o, j * seqs * GROUP : (j + 1) * seqs * GROUP, :]
            keys = cache[b, o * EACH + j, :, 0].reshape(tokens, HEAD)
            scores = lax.dot_general(
                queries, keys, (((1,), (1,)), ((), ())), preferred_element_type=jnp.float32
            )
            all_scores.append(scores[b * GROUP : (b + 1) * GROUP] * score_scale)
        alive = [live[b, pl.ds(o * EACH + j, 1), :] > 0.5 for o, j, b in pairs]
        masked = [jnp.where(a, x, FLOOR) for a, x in zip(alive, all_scores)]
        peaks = [jnp.max(x, axis=1, keepdims=True) for x in masked]
        weights = [
            jnp.where(a, jnp.exp(x - p), 0.0) for a, x, p in zip(alive, masked, peaks)
        ]
        both = []
        for weight in weights:
            high = weight.astype(jnp.bfloat16).astype(jnp.float32)
            both.append(jnp.concatenate([high, weight - high], axis=0).astype(jnp.bfloat16))
        outs = []
        for (o, j, b), w in zip(pairs, both):
            values = cache[b, o * EACH + j, :, 1].reshape(tokens, HEAD)
            out = jnp.dot(w, values, preferred_element_type=jnp.float32)
            outs.append(out[:GROUP] + out[GROUP:])
        totals = [jnp.sum(weight, axis=1, keepdims=True) for weight in weights]
        n = EACH * seqs
        return [
            (outs[k * n : (k + 1) * n], peaks[k * n : (k + 1) * n], totals[k * n : (k + 1) * n])
            for k in range(len(owners))
        ]

    def put(ref, found):
        packed = jnp.zeros((GROUP, HEAD), jnp.float32)
        outs, peaks, totals = found
        for n in range(EACH * seqs):
            ref[n] = outs[n]
            packed = jnp.where(lanes == 2 * n, peaks[n], packed)
            packed = jnp.where(lanes == 2 * n + 1, totals[n], packed)
        ref[EACH * seqs] = packed

    def stats_copy(i):
        return remote(
            stats.at[i], got_stats.at[me], st_send.at[i], st_recv.at[me], first + order[i]
        )

    for batch in ROUNDS:
        for i in batch:
            if i < last:
                wait_q(order[i])
            else:
                when_not_owner(functools.partial(wait_q, order[i]))
        results = attend([order[i] for i in batch])
        for i, found in zip(batch, results):
            put(stats.at[i], found)
            if i < last:
                c = stats_copy(i)
                c.start()
                sends.append(c)
            else:
                when_not_owner(lambda: stats_copy(last).start())

    def keep_stats():
        got_stats[me] = stats[last]

    when_owner(keep_stats)

    def finish_own():
        for i in range(1, seq_count):
            s = peer(i)
            remote(
                part_kv.at[0], got_kv.at[s], partkv_send.at[0], partkv_recv.at[s], s
            ).wait_recv()
        new_kv = got_kv[0]
        for s in range(1, seq_count):
            new_kv = new_kv + got_kv[s]
        q_rows = EACH * seqs * GROUP
        scale = own_q[q_rows : q_rows + seqs, :][:, :1]
        new_kv = (new_kv * scale).astype(jnp.bfloat16).astype(jnp.float32)
        pairs = [(j, b) for j in range(EACH) for b in range(seqs)]
        own_scores, new_values = [], []
        for j, b in pairs:
            at = (j * seqs + b) * GROUP
            query = own_q[at : at + GROUP, :]
            new_key = new_kv[b : b + 1, j * HEAD : (j + 1) * HEAD]
            own_scores.append(jnp.sum(query * new_key, axis=1, keepdims=True) * score_scale)
            new_values.append(new_kv[b : b + 1, (EACH + j) * HEAD : (EACH + j + 1) * HEAD])
        for i in range(1, seq_count):
            s = peer(i)
            remote(stats.at[0], got_stats.at[s], st_send.at[0], st_recv.at[s], s).wait_recv()
        rows = []
        packed = [got_stats[s, EACH * seqs] for s in range(seq_count)]
        for n in range(EACH * seqs):
            top = own_scores[n]
            for s in range(seq_count):
                top = jnp.maximum(top, packed[s][:, 2 * n : 2 * n + 1])
            own_weight = jnp.exp(own_scores[n] - top)
            denominator = own_weight
            numerator = own_weight * new_values[n]
            for s in range(seq_count):
                factor = jnp.exp(packed[s][:, 2 * n : 2 * n + 1] - top)
                denominator = denominator + packed[s][:, 2 * n + 1 : 2 * n + 2] * factor
                numerator = numerator + got_stats[s, n] * factor
            rows.append(numerator / denominator)
        att_all[order[last]] = jnp.concatenate(rows, axis=0).astype(jnp.bfloat16)
        for i in range(1, seq_count):
            remote(
                att_all.at[order[last]], att_all.at[order[last]], att_send.at[i], att_recv.at[order[last]], peer(i)
            ).start()

    when_owner(finish_own)

    def wait_att(g):
        remote(att_all.at[g], att_all.at[g], att_send.at[0], att_recv.at[g], peer(1)).wait_recv()

    for g in range(OWNERS):
        o_copies[g].wait()
    branch = jnp.zeros((seqs, width), jnp.float32)
    for batch in OUTPUT_ROUNDS:
        for i in batch:
            if i < last:
                wait_att(order[i])
            else:
                when_not_owner(functools.partial(wait_att, order[i]))
        for i in batch:
            att_wide[i] = att_all[order[i]].astype(jnp.float32)
        for i in batch:
            attended = jnp.concatenate(
                [
                    att_wide[i, pl.ds(j * seqs * GROUP + h, seqs, stride=GROUP), :]
                    for j in range(EACH)
                    for h in range(GROUP)
                ],
                axis=1,
            ).astype(jnp.bfloat16)
            at = pl.multiple_of(order[i] * EACH * GW, EACH * GW)
            attention_out[0, :, pl.ds(at, EACH * GW)] = attended
            branch = branch + jnp.dot(
                attended, w_o[order[i]], preferred_element_type=jnp.float32
            )
    new_hidden = (hidden[...] + branch).astype(jnp.bfloat16)
    hidden_out[0] = new_hidden

    @pl.when(section < section_count - 1)
    def _():
        hidden_send[...] = new_hidden.astype(jnp.float32)
        c = next_section_copy(section + 1)
        c.start()
        c.wait_send()

    for c in sends:
        c.wait_send()

    def drain_owner():
        for i in range(1, seq_count):
            remote(
                q_all.at[order[last]], q_all.at[order[last]], q_send.at[i], q_recv.at[order[last]], peer(i)
            ).wait_send()
            remote(
                att_all.at[order[last]], att_all.at[order[last]], att_send.at[i], att_recv.at[order[last]], peer(i)
            ).wait_send()

    def drain_other():
        part_copy(last).wait_send()
        kv_part_copy(last).wait_send()
        stats_copy(last).wait_send()

    when_owner(drain_owner)
    when_not_owner(drain_other)


def hand_on(hidden_ref, attention_ref, hidden_out, attention_out):
    hidden_out[...] = hidden_ref[...]
    attention_out[...] = attention_ref[...]


def body(hidden_in, norm_gain, qkv_weight, out_weight, memory, lengths, selected):
    seq_count = lax.axis_size("seq")
    section_count = lax.axis_size("section")
    seqs, width = hidden_in.shape
    blocks_local = memory.shape[3]
    dma = pltpu.SemaphoreType.DMA
    vmem = pl.BlockSpec(memory_space=pltpu.VMEM)
    anywhere = pl.BlockSpec(memory_space=pl.ANY)
    hidden_out, attention = pl.pallas_call(
        functools.partial(kernel, seq_count, section_count),
        out_shape=(
            jax.ShapeDtypeStruct((1, seqs, width), jnp.bfloat16),
            jax.ShapeDtypeStruct((1, seqs, HEADS * HEAD), jnp.bfloat16),
        ),
        in_specs=[
            vmem,
            vmem,
            pl.BlockSpec(memory_space=pltpu.SMEM),
            vmem,
            anywhere,
            anywhere,
            anywhere,
        ],
        out_specs=(vmem, vmem),
        scratch_shapes=[
            pltpu.VMEM((KVH, width, GW), jnp.bfloat16),
            pltpu.VMEM((width, 2 * KVH * HEAD), jnp.bfloat16),
            pltpu.VMEM((OWNERS, EACH * GW, width), jnp.bfloat16),
            pltpu.VMEM((seqs, KVH, blocks_local, 2, BLOCK, HEAD), jnp.bfloat16),
            pltpu.VMEM((seqs, width), jnp.float32),
            pltpu.VMEM((seqs, width), jnp.float32),
            pltpu.VMEM((seqs, KVH, blocks_local * BLOCK), jnp.float32),
            pltpu.VMEM((OWNERS, seqs, EACH * GW + HEAD), jnp.float32),
            pltpu.VMEM((OWNERS, seqs, 2 * EACH * HEAD), jnp.float32),
            pltpu.VMEM((seq_count, seqs, EACH * GW + HEAD), jnp.float32),
            pltpu.VMEM((seq_count, seqs, 2 * EACH * HEAD), jnp.float32),
            pltpu.VMEM((EACH * seqs * GROUP + 8, HEAD), jnp.float32),
            pltpu.VMEM((OWNERS, EACH * seqs * GROUP, HEAD), jnp.bfloat16),
            pltpu.VMEM((OWNERS, EACH * seqs + 1, GROUP, HEAD), jnp.float32),
            pltpu.VMEM((seq_count, EACH * seqs + 1, GROUP, HEAD), jnp.float32),
            pltpu.VMEM((OWNERS, EACH * seqs * GROUP, HEAD), jnp.bfloat16),
            pltpu.VMEM((OWNERS, EACH * seqs * GROUP, HEAD), jnp.float32),
            dma((KVH,)),
            dma,
            dma((OWNERS,)),
            dma,
            dma((2,)),
            dma((OWNERS,)),
            dma((seq_count,)),
            dma((OWNERS,)),
            dma((seq_count,)),
            dma((seq_count,)),
            dma((OWNERS,)),
            dma((OWNERS,)),
            dma((seq_count,)),
            dma((seq_count,)),
            dma((OWNERS,)),
        ],
        compiler_params=pltpu.CompilerParams(
            collective_id=0, has_side_effects=True, vmem_limit_bytes=56 * 1024 * 1024
        ),
    )(hidden_in, norm_gain, lengths, selected, qkv_weight, out_weight, memory)
    return pl.pallas_call(
        hand_on,
        out_shape=(
            jax.ShapeDtypeStruct(hidden_out.shape, hidden_out.dtype),
            jax.ShapeDtypeStruct(attention.shape, attention.dtype),
        ),
        in_specs=[vmem, vmem],
        out_specs=(vmem, vmem),
    )(hidden_out, attention)


def solution(mesh):
    return jax.shard_map(
        body,
        mesh=mesh,
        in_specs=(
            P("groups", "seq"),
            P("section", "seq"),
            P("section", "seq", None),
            P("section", None, "seq"),
            P("section", "groups", None, "seq", None, None, None),
            P("groups"),
            P("groups", None, None),
        ),
        out_specs=(P("section", "groups", "seq"), P("section", "groups", None)),
        check_vma=False,
    )
```
